32 devices in a mesh: rep: 2 (over y), grp: 4 (over z), tp: 2 (over x), sub: 2 (over core).
Axes of the slice: x: 2, y: 2, z: 4, core: 2. Of those that a mesh axis runs over, the one named last changes fastest.
Arguments:
- new_q: bfloat16 [4096, 8192], P(('rep', 'grp', 'sub'), 'tp'), parts along dimension 0
- new_kv: bfloat16 [2, 4096, 1024], P(None, ('rep', 'grp', 'sub'), 'tp'), parts along dimension 1
- hist_kv: bfloat16 [2, 8, 4, 4, 128, 1024], P(None, ('rep', 'grp'), None, None, 'sub', 'tp'), parts along dimension 1, may hold values from -6 to 6
- page_place: int32 [8, 16], P(('rep', 'grp')), parts along dimension 0, may hold values from 0 to 15, each once within a row
- hist_len: int32 [8], P(('rep', 'grp')), parts along dimension 0, may hold values from 1 to 2048, 4096 in all
- new_len: int32 [8], P(('rep', 'grp')), parts along dimension 0, may hold values from 128 to 512, as said below
- dec_q: bfloat16 [128, 8192], P(('rep', 'grp', 'sub'), 'tp'), parts along dimension 0
- dec_cache: bfloat16 [2, 128, 512, 1024], P(None, ('rep', 'grp', 'sub'), None, 'tp'), parts along dimension 1
- dec_len: int32 [128], P(('rep', 'grp', 'sub')), parts along dimension 0, may hold values from 64 to 512, as said below
Outputs:
- prefill_out: bfloat16 [4096, 8192], P(('rep', 'grp', 'sub'), 'tp'), parts along dimension 0
- decode_out: bfloat16 [128, 8192], P(('rep', 'grp', 'sub'), 'tp'), parts along dimension 0
The draws below stay inside these ranges and needn't reach their ends.
There are 2 independent parts, one for each index of `rep`. The reference program is written for one: setup_inputs(seed, part) draws one part's arguments, and reference() takes and returns one part's arrays. A program takes and returns all parts, laid end to end along the dimension named above; each array names one. Nothing has to cross between parts.
Inputs may be any that keep to these rules, and one draw needn't show every extreme that they name: `page_place`: each row is an ordering of the slots 0 to 15: each owner holds exactly 4 pages of every conversation. `hist_len`: some conversation has exactly 2048. `new_len`: some conversation has exactly 512. `dec_len`: some request has exactly 512.
All inputs are finite; a program needn't handle non-finite values. No bound on the sum of `hist_len` on one device may be relied on, other than what follows from the above.
Results may differ from the reference program's by a relative error of at most 0.008.
Values may be sent and summed in bfloat16 or wider, within the bound.
No kernel may reach another device: no remote copies, remote signals or barrier semaphores. Data moves between devices by JAX's collectives and lax.ppermute only.
A program may use at most 128 MiB of HBM per device.

```python
import math
import jax
import jax.numpy as jnp
import numpy as np
from jax import lax

HQ = 64
KVH = 8
HD = 128
NEW = 512
PAGE = 128
P_MAX = 16
CACHE = 512
NG = 4
CAP = 4
HIST_MAX = 2048
DEC_REQ = 64


def fresh_keys(key):
    base = jax.random.normal(jax.random.fold_in(key, 11), (NG * NEW, KVH * HD), jnp.float32)
    return base


def cache_keys(key):
    base = jax.random.normal(jax.random.fold_in(key, 31), (DEC_REQ, CACHE, KVH * HD), jnp.float32)
    return base


def draw_values(key, shape):
    return jax.random.normal(key, shape, jnp.float32)


def draw_new_kv(key, part):
    keys = fresh_keys(key)
    values = draw_values(jax.random.fold_in(key, 13), keys.shape)
    return jnp.stack([keys, values]).astype(jnp.bfloat16)


def draw_new_q(key, part):
    base = jax.random.normal(jax.random.fold_in(key, 21), (NG * NEW, HQ, HD), jnp.float32)
    return base.reshape(NG * NEW, HQ * HD).astype(jnp.bfloat16)


def draw_dec_cache(key, part):
    keys = cache_keys(key)
    values = draw_values(jax.random.fold_in(key, 33), keys.shape)
    return jnp.stack([keys, values]).astype(jnp.bfloat16)


def draw_dec_q(key, part):
    base = jax.random.normal(jax.random.fold_in(key, 41), (DEC_REQ, HQ, HD), jnp.float32)
    return base.reshape(DEC_REQ, HQ * HD).astype(jnp.bfloat16)


def draw_new_len(key, part):
    counts = jax.random.randint(jax.random.fold_in(key, 51), (NG,), NEW // 4, NEW + 1)
    chosen = jax.random.randint(jax.random.fold_in(key, 52), (), 0, NG)
    return jnp.where(jnp.arange(NG) == chosen, NEW, counts).astype(jnp.int32)


def draw_dec_len(key, part):
    counts = jax.random.randint(jax.random.fold_in(key, 61), (DEC_REQ,), CACHE // 8, CACHE + 1)
    chosen = jax.random.randint(jax.random.fold_in(key, 62), (), 0, DEC_REQ)
    return jnp.where(jnp.arange(DEC_REQ) == chosen, CACHE, counts).astype(jnp.int32)


def shard_levels(key, shape, split, smallest, largest):
    def one(position, blocks):
        heights = jax.random.uniform(jax.random.fold_in(jax.random.fold_in(key, 6), position), (blocks,), jnp.float32, smallest / len(split), largest / len(split))
        return jnp.repeat(jnp.exp(heights), shape[position] // blocks).reshape((-1,) + (1,) * (len(shape) - position - 1))

    factor_of = one(*split[0])
    for cut in split[1:]:
        factor_of = factor_of * one(*cut)
    return factor_of


def length_profile(amount, total, most, slope):
    loads = [(1 << 20) // math.isqrt(rank ** slope) + 1 for rank in range(2, amount + 1)]
    surplus, given = total - most - (amount - 1), [1] * (amount - 1)
    while surplus > 0:
        candidates = [i for i in range(amount - 1) if given[i] < most]
        pool, remaining = sum([loads[i] for i in candidates]), surplus
        for i in candidates:
            addition = min(most - given[i], max(1, remaining * loads[i] // pool), surplus)
            given[i] = given[i] + addition
            surplus = surplus - addition
    return np.array([most] + given)


def ragged(stream_key, amount, total, bound, lean):
    if amount == 2:
        one = jax.random.randint(stream_key, (), max(1, total - bound), min(bound, total - 1) + 1)
        return jnp.stack([one, total - one])
    tallies = jnp.asarray(length_profile(amount, total, bound, lean), jnp.int32)
    pairs = (amount - 1) // 2
    donor, taker = tallies[1:1 + 2 * pairs:2], tallies[2:2 + 2 * pairs:2]
    slack = jnp.minimum(donor - 1, bound - taker)
    shifted = jax.random.randint(jax.random.fold_in(stream_key, 1), (pairs,), 0, 1 << 20) % (slack + 1)
    tallies = tallies.at[1:1 + 2 * pairs:2].set(donor - shifted).at[2:2 + 2 * pairs:2].set(taker + shifted)
    return tallies[jax.random.permutation(jax.random.fold_in(stream_key, 2), amount)]


def gaussian(stream_key, extent, scale, most, shards=(), kind=jnp.bfloat16):
    level = shard_levels(stream_key, extent, shards, -0.22, 0.18) if shards else 1.0
    drawn = jax.random.normal(stream_key, extent, jnp.float32) * scale * level
    return jnp.minimum(jnp.maximum(drawn, -most), most).astype(kind)


def setup_inputs(seed: int = 0, part: int = 0) -> dict:
    splits = jax.random.split(jax.random.key(seed), 10)
    part_splits = jax.random.split(jax.random.fold_in(splits[9], part), 10)
    new_q = draw_new_q(jax.random.fold_in(jax.random.fold_in(splits[9], part), 71), part)
    new_kv = draw_new_kv(jax.random.fold_in(jax.random.fold_in(splits[9], part), 71), part)
    hist_kv = gaussian(part_splits[2], (2, NG, NG, CAP, PAGE, KVH * HD), 1.0, 6.0, ((1, 4), (4, 2), (5, 2)))
    page_place = jax.vmap(lambda own: jax.random.permutation(own, P_MAX))(jax.random.split(part_splits[3], NG)).reshape((NG, P_MAX)).astype(jnp.int32)
    hist_len = ragged(part_splits[4], NG, NG * HIST_MAX // 2, HIST_MAX, 2).astype(jnp.int32)
    new_len = draw_new_len(jax.random.fold_in(jax.random.fold_in(splits[9], part), 71), part)
    dec_q = draw_dec_q(jax.random.fold_in(jax.random.fold_in(splits[9], part), 71), part)
    dec_cache = draw_dec_cache(jax.random.fold_in(jax.random.fold_in(splits[9], part), 71), part)
    dec_len = draw_dec_len(jax.random.fold_in(jax.random.fold_in(splits[9], part), 71), part)
    return dict(new_q=new_q, new_kv=new_kv, hist_kv=hist_kv, page_place=page_place, hist_len=hist_len, new_len=new_len, dec_q=dec_q, dec_cache=dec_cache, dec_len=dec_len)


NEG = -1e30


def weigh(scores, allowed, values_form, values):
    scores = jnp.where(allowed, scores, NEG)
    top = jnp.max(scores, axis=-1, keepdims=True)
    weights = jnp.exp(scores - top)
    total = jnp.sum(weights, axis=-1)
    rounded = lax.optimization_barrier(weights.astype(jnp.bfloat16))
    mixed = jnp.einsum(values_form, rounded.astype(jnp.float32), values.astype(jnp.float32))
    return mixed / total[..., None]


def reference(new_q, new_kv, hist_kv, page_place, hist_len, new_len, dec_q, dec_cache, dec_len):
    group = HQ // KVH
    scale = HD ** -0.5
    positions = jnp.arange(NEW, dtype=jnp.int32)
    hist_pos = jnp.arange(P_MAX * PAGE, dtype=jnp.int32)

    def one_conv(conv):
        owned = jnp.take(hist_kv, conv, axis=2).reshape(2, NG * CAP, PAGE, KVH, HD)
        place = jnp.take(page_place, conv, axis=0)
        ordered = jnp.take(owned, place, axis=1).reshape(2, P_MAX * PAGE, KVH, HD)
        fresh = lax.dynamic_slice_in_dim(new_kv, conv * NEW, NEW, 1).reshape(2, NEW, KVH, HD)
        keys = jnp.concatenate([ordered[0], fresh[0]], axis=0)
        values = jnp.concatenate([ordered[1], fresh[1]], axis=0)
        limit = jnp.take(hist_len, conv)
        count = jnp.take(new_len, conv)
        seen_hist = jnp.broadcast_to((hist_pos < limit)[None, :], (NEW, P_MAX * PAGE))
        seen_new = (positions[None, :] <= positions[:, None]) & (positions[None, :] < count)
        allowed = jnp.concatenate([seen_hist, seen_new], axis=1)
        queries = lax.dynamic_slice_in_dim(new_q, conv * NEW, NEW, 0).reshape(NEW, KVH, group, HD)
        scores = jnp.einsum('qkgd,skd->kgqs', queries.astype(jnp.float32), keys.astype(jnp.float32)) * scale
        mixed = weigh(scores, allowed[None, None], 'kgqs,skd->kgqd', values)
        out = jnp.transpose(mixed, (2, 0, 1, 3)).reshape(NEW, HQ * HD)
        out = jnp.where((positions < count)[:, None], out, 0.0)
        return out.astype(jnp.bfloat16)

    prefill_out = lax.map(one_conv, jnp.arange(NG, dtype=jnp.int32)).reshape(NG * NEW, HQ * HD)

    requests = dec_q.shape[0]
    dq = dec_q.reshape(requests, KVH, group, HD).astype(jnp.float32)
    dkeys = dec_cache[0].reshape(requests, CACHE, KVH, HD).astype(jnp.float32)
    dvalues = dec_cache[1].reshape(requests, CACHE, KVH, HD)
    dscores = jnp.einsum('rkgd,rskd->rkgs', dq, dkeys) * scale
    dallowed = (jnp.arange(CACHE, dtype=jnp.int32)[None, :] < dec_len[:, None])[:, None, None, :]
    dmixed = weigh(dscores, dallowed, 'rkgs,rskd->rkgd', dvalues)
    decode_out = dmixed.reshape(requests, HQ * HD).astype(jnp.bfloat16)
    return prefill_out, decode_out
```

```python
import functools
import math

import jax
import jax.numpy as jnp
from jax import lax
from jax.experimental import pallas as pl
from jax.experimental.pallas import tpu as pltpu
from jax.sharding import PartitionSpec as P

HQ = 64
KVH = 8
HD = 128
PAGE = 128
GROUP = HQ // KVH
NEG = -1e30
COEF = (HD**-0.5) * math.log2(math.e)


def dot_t(a, b):
    return lax.dot_general(a, b, (((1,), (1,)), ((), ())), preferred_element_type=jnp.float32)


def dot_n(a, b):
    return lax.dot_general(a, b, (((1,), (0,)), ((), ())), preferred_element_type=jnp.float32)


def local_kernel(info, q_ref, *refs, parts):
    kv_refs, (acc_out, ml_out) = refs[:parts], refs[parts:]
    rows = q_ref.shape[0]
    q_base, count = info[0], info[1]
    keys = jnp.concatenate([r[0] for r in kv_refs], axis=0)
    values = jnp.concatenate([r[1] for r in kv_refs], axis=0)
    q_pos = q_base + lax.broadcasted_iota(jnp.int32, (rows, rows), 0)
    biases = []
    for p in range(parts):
        k_pos = info[2 + p] + lax.broadcasted_iota(jnp.int32, (rows, rows), 1)
        biases.append(jnp.where((k_pos <= q_pos) & (k_pos < count), 0.0, NEG))
    bias = jnp.concatenate(biases, axis=1)
    lane = lax.broadcasted_iota(jnp.int32, (rows, HD), 1)
    ml = jnp.zeros((rows, HD), jnp.float32)
    for h in range(GROUP):
        cols = slice(h * HD, (h + 1) * HD)
        scores = dot_t(q_ref[:, cols], keys) * COEF + bias
        top = jnp.max(scores, axis=1, keepdims=True)
        weights = jnp.exp2(scores - top)
        total = jnp.sum(weights, axis=1, keepdims=True)
        acc_out[:, cols] = dot_n(weights.astype(jnp.bfloat16), values)
        ml = jnp.where(lane == h, top, ml)
        ml = jnp.where(lane == GROUP + h, total, ml)
    ml_out[0] = ml


def page_kernel(info, q_ref, *refs, parts, offset, last):
    kv_refs, (acc_in, ml_in), outs = refs[:parts], refs[parts : parts + 2], refs[parts + 2 :]
    rows = q_ref.shape[0]
    slots, tokens = kv_refs[0].shape[1], kv_refs[0].shape[2]
    total_keys = parts * slots * tokens
    base = 2 + parts + offset * parts * slots
    counts = [info[base + i] for i in range(parts * slots)]
    any_keys = functools.reduce(jnp.add, counts) > 0

    def write(cols, acc, total):
        q_pos = info[0] + lax.broadcasted_iota(jnp.int32, (rows, HD), 0)
        outs[0][:, cols] = jnp.where(q_pos < info[1], acc / total, 0.0).astype(jnp.bfloat16)

    @pl.when(any_keys)
    def _():
        keys = jnp.concatenate([r[0].reshape(slots * tokens, HD) for r in kv_refs], axis=0)
        values = jnp.concatenate([r[1].reshape(slots * tokens, HD) for r in kv_refs], axis=0)
        token = lax.broadcasted_iota(jnp.int32, (1, total_keys), 1)
        limit = jnp.zeros((1, total_keys), jnp.int32)
        for i, c in enumerate(counts):
            limit = jnp.where(token >= i * tokens, i * tokens + c, limit)
        bias = jnp.where(token < limit, 0.0, NEG)
        lane = lax.broadcasted_iota(jnp.int32, (rows, HD), 1)
        ml_old = ml_in[0]
        ml = ml_old
        for h in range(GROUP):
            cols = slice(h * HD, (h + 1) * HD)
            scores = dot_t(q_ref[:, cols], keys) * COEF + bias
            old = ml_old[:, h : h + 1]
            top = jnp.maximum(old, jnp.max(scores, axis=1, keepdims=True))
            weights = jnp.exp2(scores - top)
            factor = jnp.exp2(old - top)
            total = ml_old[:, GROUP + h : GROUP + h + 1] * factor + jnp.sum(
                weights, axis=1, keepdims=True
            )
            acc = acc_in[:, cols] * factor + dot_n(weights.astype(jnp.bfloat16), values)
            if last:
                write(cols, acc, total)
            else:
                outs[0][:, cols] = acc
                ml = jnp.where(lane == h, top, ml)
                ml = jnp.where(lane == GROUP + h, total, ml)
        if not last:
            outs[1][0] = ml

    @pl.when(jnp.logical_not(any_keys))
    def _():
        for h in range(GROUP):
            cols = slice(h * HD, (h + 1) * HD)
            if last:
                write(cols, acc_in[:, cols], ml_in[0][:, GROUP + h : GROUP + h + 1])
            else:
                outs[0][:, cols] = acc_in[:, cols]
        if not last:
            outs[1][0] = ml_in[0]


def decode_kernel(lens, q_ref, kv_ref, out_ref):
    r = pl.program_id(0)
    cached = kv_ref.shape[2]
    token = lax.broadcasted_iota(jnp.int32, (1, cached), 1)
    bias = jnp.where(token < lens[r], 0.0, NEG)
    for k in range(kv_ref.shape[3] // HD):
        cols = slice(k * HD, (k + 1) * HD)
        heads = slice(k * GROUP, (k + 1) * GROUP)
        scores = dot_t(q_ref[0, heads, :], kv_ref[0, 0, :, cols]) * COEF + bias
        top = jnp.max(scores, axis=1, keepdims=True)
        weights = jnp.exp2(scores - top)
        total = jnp.sum(weights, axis=1, keepdims=True)
        mixed = dot_n(weights.astype(jnp.bfloat16), kv_ref[1, 0, :, cols])
        out_ref[0, heads, :] = (mixed / total).astype(jnp.bfloat16)


def cost(rows, heads, keys, nbytes):
    return pl.CostEstimate(
        flops=4 * rows * heads * keys * HD, transcendentals=rows * heads * keys, bytes_accessed=nbytes
    )


def run_local(info, q, kvs):
    rows = q.shape[0]
    kv_local = kvs[0].shape[2] // HD
    wide = GROUP * HD
    return pl.pallas_call(
        functools.partial(local_kernel, parts=len(kvs)),
        grid_spec=pltpu.PrefetchScalarGridSpec(
            num_scalar_prefetch=1,
            grid=(kv_local,),
            in_specs=[pl.BlockSpec((rows, wide), lambda k, s: (0, k))]
            + [pl.BlockSpec((2, rows, HD), lambda k, s: (0, 0, k)) for _ in kvs],
            out_specs=[
                pl.BlockSpec((rows, wide), lambda k, s: (0, k)),
                pl.BlockSpec((1, rows, HD), lambda k, s: (k, 0, 0)),
            ],
        ),
        out_shape=[
            jax.ShapeDtypeStruct((rows, kv_local * wide), jnp.float32),
            jax.ShapeDtypeStruct((kv_local, rows, HD), jnp.float32),
        ],
        cost_estimate=cost(rows, kv_local * GROUP, rows * len(kvs), rows * kv_local * wide * 6),
        name="local_stage",
    )(info, q, *kvs)


def run_pages(info, q, kvs, acc, ml, offset, last):
    rows = q.shape[0]
    slots, tokens = kvs[0].shape[1], kvs[0].shape[2]
    kv_local = kvs[0].shape[3] // HD
    wide = GROUP * HD
    acc_spec = pl.BlockSpec((rows, wide), lambda k, s: (0, k))
    ml_spec = pl.BlockSpec((1, rows, HD), lambda k, s: (k, 0, 0))
    parts = len(kvs)
    if last:
        out_specs = [acc_spec]
        out_shape = [jax.ShapeDtypeStruct(acc.shape, jnp.bfloat16)]
        aliases = {}
    else:
        out_specs = [acc_spec, ml_spec]
        out_shape = [
            jax.ShapeDtypeStruct(acc.shape, jnp.float32),
            jax.ShapeDtypeStruct(ml.shape, jnp.float32),
        ]
        aliases = {2 + parts: 0, 3 + parts: 1}
    return pl.pallas_call(
        functools.partial(page_kernel, parts=parts, offset=offset, last=last),
        grid_spec=pltpu.PrefetchScalarGridSpec(
            num_scalar_prefetch=1,
            grid=(kv_local,),
            in_specs=[pl.BlockSpec((rows, wide), lambda k, s: (0, k))]
            + [pl.BlockSpec((2, slots, tokens, HD), lambda k, s: (0, 0, 0, k)) for _ in kvs]
            + [acc_spec, ml_spec],
            out_specs=out_specs,
        ),
        out_shape=out_shape,
        input_output_aliases=aliases,
        cost_estimate=cost(
            rows, kv_local * GROUP, parts * slots * tokens, rows * kv_local * wide * 10
        ),
        name="page_stage_last" if last else "page_stage",
    )(info, q, *kvs, acc, ml)


def run_decode(dec_q, dec_cache, dec_len):
    requests, width = dec_q.shape
    heads = width // HD
    cached, kv_width = dec_cache.shape[2], dec_cache.shape[3]
    out = pl.pallas_call(
        decode_kernel,
        grid_spec=pltpu.PrefetchScalarGridSpec(
            num_scalar_prefetch=1,
            grid=(requests,),
            in_specs=[
                pl.BlockSpec((1, heads, HD), lambda r, s: (r, 0, 0)),
                pl.BlockSpec((2, 1, cached, kv_width), lambda r, s: (0, r, 0, 0)),
            ],
            out_specs=pl.BlockSpec((1, heads, HD), lambda r, s: (r, 0, 0)),
        ),
        out_shape=jax.ShapeDtypeStruct((requests, heads, HD), jnp.bfloat16),
        cost_estimate=cost(requests, heads, cached, 2 * dec_cache.size),
        name="decode_stage",
    )(dec_len, dec_q.reshape(requests, heads, HD), dec_cache)
    return out.reshape(requests, width)


def shift(block, axis, distance):
    size = lax.axis_size(axis)
    return lax.ppermute(block, axis, [(i, (i + distance) % size) for i in range(size)])


def attend(new_q, new_kv, hist_kv, page_place, hist_len, new_len, dec_q, dec_cache, dec_len):
    rows = new_q.shape[0]
    owners, subs = lax.axis_size("grp"), lax.axis_size("sub")
    own, sub = lax.axis_index("grp"), lax.axis_index("sub")
    slots, tokens = hist_kv.shape[3], hist_kv.shape[4]

    order = sorted(range(1, owners), key=lambda k: (-min(k, owners - k), k))
    arrived = {}
    for k in order:
        dest = lax.rem(own + k, owners)
        piece = lax.dynamic_slice_in_dim(hist_kv, dest, 1, 2)[:, 0, 0]
        arrived[k] = shift(piece, "grp", k)
    arrived[0] = lax.dynamic_slice_in_dim(hist_kv, own, 1, 2)[:, 0, 0]

    i32 = jnp.int32
    place = page_place[0]
    slot_id = lax.rem(own - jnp.arange(owners, dtype=i32) + owners, owners)[:, None] * slots
    slot_id = slot_id + jnp.arange(slots, dtype=i32)[None, :]
    page = jnp.sum(
        jnp.where(
            place[None, None, :] == slot_id[:, :, None],
            jnp.arange(place.shape[0], dtype=i32)[None, None, :],
            0,
        ),
        axis=2,
    )
    half = lax.rem(sub - jnp.arange(subs, dtype=i32) + subs, subs)
    start = page[:, None, :] * PAGE + half[None, :, None] * tokens
    visible = jnp.clip(hist_len[0] - start, 0, tokens)
    info = jnp.concatenate(
        [(sub * rows).reshape(1), new_len, half * rows, visible.reshape(-1)]
    ).astype(i32)

    def both(block):
        return [block] + [shift(block, "sub", s) for s in range(1, subs)]

    decode_out = run_decode(dec_q, dec_cache, dec_len)
    acc, ml = run_local(info, new_q, both(new_kv))
    stages = [0] + order
    for k in stages:
        last = k == stages[-1]
        block = arrived[k]
        if k:
            block, ml, decode_out = lax.optimization_barrier((block, ml, decode_out))
        found = run_pages(info, new_q, both(block), acc, ml, k, last)
        if last:
            prefill_out = found[0]
        else:
            acc, ml = found
    return (prefill_out, decode_out)


def solution(mesh):
    in_specs = (
        P(("rep", "grp", "sub"), "tp"),
        P(None, ("rep", "grp", "sub"), "tp"),
        P(None, ("rep", "grp"), None, None, "sub", "tp"),
        P(("rep", "grp"), None),
        P(("rep", "grp")),
        P(("rep", "grp")),
        P(("rep", "grp", "sub"), "tp"),
        P(None, ("rep", "grp", "sub"), None, "tp"),
        P(("rep", "grp", "sub")),
    )
    out_specs = (P(("rep", "grp", "sub"), "tp"), P(("rep", "grp", "sub"), "tp"))
    return jax.shard_map(attend, mesh=mesh, in_specs=in_specs, out_specs=out_specs, check_vma=False)
```

```python
import functools
import math

import jax
import jax.numpy as jnp
from jax import lax
from jax.experimental import pallas as pl
from jax.experimental.pallas import tpu as pltpu
from jax.sharding import PartitionSpec as P

HQ = 64
KVH = 8
HD = 128
PAGE = 128
GROUP = HQ // KVH
NEG = -1e30
COEF = (HD**-0.5) * math.log2(math.e)


def dot_t(a, b):
    return lax.dot_general(a, b, (((1,), (1,)), ((), ())), preferred_element_type=jnp.float32)


def dot_n(a, b):
    return lax.dot_general(a, b, (((1,), (0,)), ((), ())), preferred_element_type=jnp.float32)


def local_kernel(info, q_ref, *refs, parts):
    kv_refs, (acc_out, ml_out) = refs[:parts], refs[parts:]
    rows = q_ref.shape[0]
    q_base, count = info[0], info[1]
    keys = jnp.concatenate([r[0] for r in kv_refs], axis=0)
    values = jnp.concatenate([r[1] for r in kv_refs], axis=0).T
    q_pos = q_base + lax.broadcasted_iota(jnp.int32, (rows, rows), 1)
    biases = []
    for p in range(parts):
        k_pos = info[2 + p] + lax.broadcasted_iota(jnp.int32, (rows, rows), 0)
        biases.append(jnp.where((k_pos <= q_pos) & (k_pos < count), 0.0, NEG))
    bias = jnp.concatenate(biases, axis=0)
    raw = dot_t(keys, q_ref[:, :HD])
    for h in range(GROUP):
        cols = slice(h * HD, (h + 1) * HD)
        scores = raw * COEF + bias
        if h + 1 < GROUP:
            raw = dot_t(keys, q_ref[:, (h + 1) * HD : (h + 2) * HD])
        top = jnp.max(scores, axis=0, keepdims=True)
        weights = jnp.exp2(scores - top)
        ml_out[0, h : h + 1, :] = top
        ml_out[0, GROUP + h : GROUP + h + 1, :] = jnp.sum(weights, axis=0, keepdims=True)
        acc_out[cols, :] = dot_n(values, weights.astype(jnp.bfloat16))


def page_kernel(info, q_ref, *refs, parts, offset, last):
    kv_refs, (acc_in, ml_in), outs = refs[:parts], refs[parts : parts + 2], refs[parts + 2 :]
    rows = q_ref.shape[0]
    slots, tokens = kv_refs[0].shape[1], kv_refs[0].shape[2]
    base = 2 + parts + offset * parts * slots
    counts = [info[base + i] for i in range(parts * slots)]
    any_keys = functools.reduce(jnp.add, counts) > 0

    def write(cols, acc, total):
        q_pos = info[0] + lax.broadcasted_iota(jnp.int32, (rows, HD), 0)
        mixed = (acc / total).T
        outs[0][:, cols] = jnp.where(q_pos < info[1], mixed, 0.0).astype(jnp.bfloat16)

    @pl.when(any_keys)
    def _():
        keys = jnp.concatenate([r[0].reshape(slots * tokens, HD) for r in kv_refs], axis=0)
        values = jnp.concatenate([r[1].reshape(slots * tokens, HD) for r in kv_refs], axis=0).T
        token = lax.broadcasted_iota(jnp.int32, (tokens, rows), 0)
        bias = jnp.concatenate([jnp.where(token < c, 0.0, NEG) for c in counts], axis=0)
        raw = dot_t(keys, q_ref[:, :HD])
        for h in range(GROUP):
            cols = slice(h * HD, (h + 1) * HD)
            scores = raw * COEF + bias
            if h + 1 < GROUP:
                raw = dot_t(keys, q_ref[:, (h + 1) * HD : (h + 2) * HD])
            old = ml_in[0, h : h + 1, :]
            top = jnp.maximum(old, jnp.max(scores, axis=0, keepdims=True))
            weights = jnp.exp2(scores - top)
            factor = jnp.exp2(old - top)
            total = ml_in[0, GROUP + h : GROUP + h + 1, :] * factor + jnp.sum(
                weights, axis=0, keepdims=True
            )
            acc = acc_in[cols, :] * factor + dot_n(values, weights.astype(jnp.bfloat16))
            if last:
                write(cols, acc, total)
            else:
                outs[0][cols, :] = acc
                outs[1][0, h : h + 1, :] = top
                outs[1][0, GROUP + h : GROUP + h + 1, :] = total

    @pl.when(jnp.logical_not(any_keys))
    def _():
        for h in range(GROUP):
            cols = slice(h * HD, (h + 1) * HD)
            if last:
                write(cols, acc_in[cols, :], ml_in[0, GROUP + h : GROUP + h + 1, :])
            else:
                outs[0][cols, :] = acc_in[cols, :]
        if not last:
            outs[1][...] = ml_in[...]


def decode_kernel(lens, q_ref, kv_ref, out_ref):
    r = pl.program_id(0)
    cached = kv_ref.shape[2]
    token = lax.broadcasted_iota(jnp.int32, (1, cached), 1)
    bias = jnp.where(token < lens[r], 0.0, NEG)
    for k in range(kv_ref.shape[3] // HD):
        cols = slice(k * HD, (k + 1) * HD)
        heads = slice(k * GROUP, (k + 1) * GROUP)
        scores = dot_t(q_ref[0, heads, :], kv_ref[0, 0, :, cols]) * COEF + bias
        top = jnp.max(scores, axis=1, keepdims=True)
        weights = jnp.exp2(scores - top)
        total = jnp.sum(weights, axis=1, keepdims=True)
        mixed = dot_n(weights.astype(jnp.bfloat16), kv_ref[1, 0, :, cols])
        out_ref[0, heads, :] = (mixed / total).astype(jnp.bfloat16)


def cost(rows, heads, keys, nbytes):
    return pl.CostEstimate(
        flops=4 * rows * heads * keys * HD, transcendentals=rows * heads * keys, bytes_accessed=nbytes
    )


def run_local(info, q, kvs):
    rows = q.shape[0]
    kv_local = kvs[0].shape[2] // HD
    wide = GROUP * HD
    return pl.pallas_call(
        functools.partial(local_kernel, parts=len(kvs)),
        grid_spec=pltpu.PrefetchScalarGridSpec(
            num_scalar_prefetch=1,
            grid=(kv_local,),
            in_specs=[pl.BlockSpec((rows, wide), lambda k, s: (0, k))]
            + [pl.BlockSpec((2, rows, HD), lambda k, s: (0, 0, k)) for _ in kvs],
            out_specs=[
                pl.BlockSpec((wide, rows), lambda k, s: (k, 0)),
                pl.BlockSpec((1, 2 * GROUP, rows), lambda k, s: (k, 0, 0)),
            ],
        ),
        out_shape=[
            jax.ShapeDtypeStruct((kv_local * wide, rows), jnp.float32),
            jax.ShapeDtypeStruct((kv_local, 2 * GROUP, rows), jnp.float32),
        ],
        cost_estimate=cost(rows, kv_local * GROUP, rows * len(kvs), rows * kv_local * wide * 6),
        name="local_stage",
    )(info, q, *kvs)


def run_pages(info, q, kvs, acc, ml, offset, last):
    rows = q.shape[0]
    slots, tokens = kvs[0].shape[1], kvs[0].shape[2]
    kv_local = kvs[0].shape[3] // HD
    wide = GROUP * HD
    q_spec = pl.BlockSpec((rows, wide), lambda k, s: (0, k))
    acc_spec = pl.BlockSpec((wide, rows), lambda k, s: (k, 0))
    ml_spec = pl.BlockSpec((1, 2 * GROUP, rows), lambda k, s: (k, 0, 0))
    parts = len(kvs)
    if last:
        out_specs = [q_spec]
        out_shape = [jax.ShapeDtypeStruct(q.shape, jnp.bfloat16)]
        aliases = {}
    else:
        out_specs = [acc_spec, ml_spec]
        out_shape = [
            jax.ShapeDtypeStruct(acc.shape, jnp.float32),
            jax.ShapeDtypeStruct(ml.shape, jnp.float32),
        ]
        aliases = {2 + parts: 0, 3 + parts: 1}
    return pl.pallas_call(
        functools.partial(page_kernel, parts=parts, offset=offset, last=last),
        grid_spec=pltpu.PrefetchScalarGridSpec(
            num_scalar_prefetch=1,
            grid=(kv_local,),
            in_specs=[pl.BlockSpec((rows, wide), lambda k, s: (0, k))]
            + [pl.BlockSpec((2, slots, tokens, HD), lambda k, s: (0, 0, 0, k)) for _ in kvs]
            + [acc_spec, ml_spec],
            out_specs=out_specs,
        ),
        out_shape=out_shape,
        input_output_aliases=aliases,
        cost_estimate=cost(
            rows, kv_local * GROUP, parts * slots * tokens, rows * kv_local * wide * 10
        ),
        name="page_stage_last" if last else "page_stage",
    )(info, q, *kvs, acc, ml)


def run_decode(dec_q, dec_cache, dec_len):
    requests, width = dec_q.shape
    heads = width // HD
    cached, kv_width = dec_cache.shape[2], dec_cache.shape[3]
    out = pl.pallas_call(
        decode_kernel,
        grid_spec=pltpu.PrefetchScalarGridSpec(
            num_scalar_prefetch=1,
            grid=(requests,),
            in_specs=[
                pl.BlockSpec((1, heads, HD), lambda r, s: (r, 0, 0)),
                pl.BlockSpec((2, 1, cached, kv_width), lambda r, s: (0, r, 0, 0)),
            ],
            out_specs=pl.BlockSpec((1, heads, HD), lambda r, s: (r, 0, 0)),
        ),
        out_shape=jax.ShapeDtypeStruct((requests, heads, HD), jnp.bfloat16),
        cost_estimate=cost(requests, heads, cached, 2 * dec_cache.size),
        name="decode_stage",
    )(dec_len, dec_q.reshape(requests, heads, HD), dec_cache)
    return out.reshape(requests, width)


def shift(block, axis, distance):
    size = lax.axis_size(axis)
    return lax.ppermute(block, axis, [(i, (i + distance) % size) for i in range(size)])


def attend(new_q, new_kv, hist_kv, page_place, hist_len, new_len, dec_q, dec_cache, dec_len):
    rows = new_q.shape[0]
    owners, subs = lax.axis_size("grp"), lax.axis_size("sub")
    own, sub = lax.axis_index("grp"), lax.axis_index("sub")
    slots, tokens = hist_kv.shape[3], hist_kv.shape[4]

    order = sorted(range(1, owners), key=lambda k: (-min(k, owners - k), k))
    arrived = {}
    for k in order:
        dest = lax.rem(own + k, owners)
        piece = lax.dynamic_slice_in_dim(hist_kv, dest, 1, 2)[:, 0, 0]
        arrived[k] = shift(piece, "grp", k)
    arrived[0] = lax.dynamic_slice_in_dim(hist_kv, own, 1, 2)[:, 0, 0]

    i32 = jnp.int32
    place = page_place[0]
    slot_id = lax.rem(own - jnp.arange(owners, dtype=i32) + owners, owners)[:, None] * slots
    slot_id = slot_id + jnp.arange(slots, dtype=i32)[None, :]
    page = jnp.sum(
        jnp.where(
            place[None, None, :] == slot_id[:, :, None],
            jnp.arange(place.shape[0], dtype=i32)[None, None, :],
            0,
        ),
        axis=2,
    )
    half = lax.rem(sub - jnp.arange(subs, dtype=i32) + subs, subs)
    start = page[:, None, :] * PAGE + half[None, :, None] * tokens
    visible = jnp.clip(hist_len[0] - start, 0, tokens)
    info = jnp.concatenate(
        [(sub * rows).reshape(1), new_len, half * rows, visible.reshape(-1)]
    ).astype(i32)

    def both(block):
        return [block] + [shift(block, "sub", s) for s in range(1, subs)]

    decode_out = run_decode(dec_q, dec_cache, dec_len)
    acc, ml = run_local(info, new_q, both(new_kv))
    stages = [0] + order
    for k in stages:
        last = k == stages[-1]
        block = arrived[k]
        if k:
            block, ml, decode_out = lax.optimization_barrier((block, ml, decode_out))
        found = run_pages(info, new_q, both(block), acc, ml, k, last)
        if last:
            prefill_out = found[0]
        else:
            acc, ml = found
    return (prefill_out, decode_out)


def solution(mesh):
    in_specs = (
        P(("rep", "grp", "sub"), "tp"),
        P(None, ("rep", "grp", "sub"), "tp"),
        P(None, ("rep", "grp"), None, None, "sub", "tp"),
        P(("rep", "grp"), None),
        P(("rep", "grp")),
        P(("rep", "grp")),
        P(("rep", "grp", "sub"), "tp"),
        P(None, ("rep", "grp", "sub"), None, "tp"),
        P(("rep", "grp", "sub")),
    )
    out_specs = (P(("rep", "grp", "sub"), "tp"), P(("rep", "grp", "sub"), "tp"))
    return jax.shard_map(attend, mesh=mesh, in_specs=in_specs, out_specs=out_specs, check_vma=False)
```
